32 devices in a mesh: exp: 8 (over z, y), tp: 4 (over x, core).
Axes of the slice: x: 2, y: 2, z: 4, core: 2. Of those that a mesh axis runs over, the one named last changes fastest.
Arguments:
- tokens: bfloat16 [2048, 2048], P('exp'), may hold values from -6 to 6
- cotangent: bfloat16 [2048, 2048], P('exp'), may hold values from -12 to 12
- seq_start: int32 [2048], P('exp'), may hold values from 0 to 248, as said below
- routes: int32 [2048, 8], P('exp'), may hold values from 0 to 31, all different within a row; in each aligned block of 256 rows (0 to 255, 256 to 511, ...) at most 96 rows name the same one
- norm1_gain: float32 [2048], replicated, may hold values from 0.25 to 1.75
- norm2_gain: float32 [2048], replicated, may hold values from 0.25 to 1.75
- q_gain: float32 [128], replicated, may hold values from 0.25 to 1.75
- k_gain: float32 [128], replicated, may hold values from 0.25 to 1.75
- query_matrix: bfloat16 [2048, 4096], P(None, 'tp'), may hold values from -0.125 to 0.125
- key_matrix: bfloat16 [2048, 512], P(None, 'tp'), may hold values from -0.125 to 0.125
- value_matrix: bfloat16 [2048, 512], P(None, 'tp'), may hold values from -0.125 to 0.125
- output_matrix: bfloat16 [2048, 4096], P(None, 'tp'), may hold values from -0.75 to 0.75
- w_router: bfloat16 [2048, 32], replicated, may hold values from -0.125 to 0.125
- w_gate: bfloat16 [32, 2048, 768], P('exp', None, 'tp'), may hold values from -0.125 to 0.125
- w_up: bfloat16 [32, 2048, 768], P('exp', None, 'tp'), may hold values from -0.125 to 0.125
- w_down: bfloat16 [32, 768, 2048], P('exp', 'tp'), may hold values from -0.4375 to 0.4375
Outputs:
- layer_out: bfloat16 [2048, 2048], P('exp')
- grad_tokens: bfloat16 [2048, 2048], P('exp')
- grad_norm1: float32 [2048], replicated
- grad_norm2: float32 [2048], replicated
- grad_q_gain: float32 [128], replicated
- grad_k_gain: float32 [128], replicated
- grad_query: float32 [2048, 4096], P('exp', 'tp')
- grad_key: float32 [2048, 512], P('exp', 'tp')
- grad_value: float32 [2048, 512], P('exp', 'tp')
- grad_out: float32 [2048, 4096], P('exp', 'tp')
- grad_router: float32 [2048, 32], P('exp')
- grad_gate: float32 [32, 2048, 768], P('exp', None, 'tp')
- grad_up: float32 [32, 2048, 768], P('exp', None, 'tp')
- grad_down: float32 [32, 768, 2048], P('exp', 'tp')
The draws below stay inside these ranges and needn't reach their ends.
Inputs may be any that keep to these rules, and one draw needn't show every extreme that they name: Sequences never cross a block of 256 rows; each block begins with a sequence of exactly 128 rows and no sequence is longer; seq_start never falls within a block and is at most the row's own index there; each block's last sequence begins at row 248. `routes`: each token names 8 different experts; among the 256 rows of one index of exp no expert is named by more than 96 rows, a bound that some block reaches.
All inputs are finite; a program needn't handle non-finite values.
Results may differ from the reference program's by a relative error of at most 0.022.
Values may be sent and summed in bfloat16 or wider, within the bound.
A program may use at most 320 MiB of HBM per device.

```python
import math
import jax
import jax.numpy as jnp
import numpy as np
from jax import lax

MODEL_DIMENSION = 2048
QUERY_HEADS = 32
KEY_VALUE_HEADS = 4
HEAD_DIMENSION = 128
FFE = 768
TOPK = 8
TOKENS_PER_SHARD = 256
EXPERTS = 32
TOKEN_TOTAL = 2048
SEQ_MAX = 128
TAIL = 8
CAP = 96
N_EXP = 8
N_TP = 4


def draw_seq_start(key, part):
    local_pos = jnp.arange(TOKEN_TOTAL) % TOKENS_PER_SHARD
    tosses = jax.random.randint(key, (TOKEN_TOTAL,), 0, 2)
    boundary = (local_pos == 0) | (local_pos == SEQ_MAX) | (local_pos == TOKENS_PER_SHARD - TAIL) | (local_pos > SEQ_MAX) & (local_pos % TAIL == 0) & (tosses == 1)
    markers = jnp.where(boundary, local_pos, 0).reshape(TOKEN_TOTAL // TOKENS_PER_SHARD, TOKENS_PER_SHARD)
    return lax.cummax(markers, axis=1).reshape(TOKEN_TOTAL).astype(jnp.int32)


def draw_cotangent(key, part):
    block_of = (jnp.arange(TOKEN_TOTAL) // TOKENS_PER_SHARD).astype(jnp.float32)
    rising = 1.0 + 2.0 * block_of / max(TOKEN_TOTAL // TOKENS_PER_SHARD - 1, 1)
    raw_values = jnp.clip(jax.random.normal(key, (TOKEN_TOTAL, MODEL_DIMENSION), jnp.float32), -4.0, 4.0)
    return (raw_values * rising[:, None]).astype(jnp.bfloat16)


def block_scale(own_key, shape, shards, least, high):
    level, own = 1.0, jax.random.fold_in(own_key, 6)
    for position, shards_of in shards:
        draws = jnp.exp(jax.random.uniform(jax.random.fold_in(own, position), (shards_of,), jnp.float32, least / len(shards), high / len(shards)))
        level = level * jnp.repeat(draws, shape[position] // shards_of).reshape([-1 if axis == position else 1 for axis in range(len(shape))])
    return level


def shared_out(own_key, own, number, rows, count, top, reach, skew):
    ranking = jax.random.permutation(own_key, count)
    packed, usual = load_shares(count, rows * top, reach, skew, True), load_shares(count, rows * top, reach, skew, False)
    places = jnp.arange(count)

    def named(tallies, offset_by):
        used = int((tallies > 0).sum())
        fixed = max(1, used // 4)
        moved = fixed + (places - fixed + offset_by * (used - fixed)) % max(1, count - fixed)
        return jnp.zeros((count,), jnp.int32).at[ranking[jnp.where(places < fixed, places, moved)]].set(jnp.asarray(tallies, jnp.int32))

    tallies = jnp.where(number % 4 == 0, named(packed, number // 4), named(usual, number - number // 4 - 1))
    mixed = jax.random.permutation(jax.random.fold_in(own, 3), count)
    source_of, taker = mixed[0:count // 2 * 2:2], mixed[1:count // 2 * 2:2]
    margin = jnp.minimum(tallies[source_of] - 1, reach - tallies[taker]) // 2
    margin = jnp.where((source_of == ranking[0]) | (taker == ranking[0]) | (tallies[taker] == 0), 0, jnp.maximum(margin, 0))
    moved = jax.random.randint(jax.random.fold_in(own, 4), (count // 2,), 0, 1 << 20) % (margin + 1)
    tallies = tallies.at[source_of].add(-moved).at[taker].add(moved)
    labels = jnp.searchsorted(jnp.cumsum(tallies), jnp.arange(rows * top), side="right").astype(jnp.int32)
    grid = labels.reshape(top, rows).T
    grid = grid[jax.random.permutation(jax.random.fold_in(own, 1), rows)]
    offset_by = jax.random.randint(jax.random.fold_in(own, 2), (rows, 1), 0, top)
    return jnp.take_along_axis(grid, (jnp.arange(top)[None, :] + offset_by) % top, axis=1)


def load_shares(count, total, reach, slope, full):
    weights = [(1 << 20) // math.isqrt(grade ** slope) + 1 for grade in range(1, count + 1)]
    largest = reach if full else min(reach, max(-(-total // count), total * weights[0] // sum(weights)))
    least = 1 if total - largest >= count - 1 else 0
    holding, rest = [largest] + [least] * (count - 1), total - largest - least * (count - 1)
    while rest > 0:
        candidates = [i for i in range(1, count) if holding[i] < largest] or [i for i in range(1, count) if holding[i] < reach]
        whole, budget = sum([weights[i] for i in candidates]), rest
        for i in candidates:
            extra = min(reach - holding[i], max(1, budget * weights[i] // whole), rest)
            holding[i] = holding[i] + extra
            rest = rest - extra
    return np.array(holding)


def gaussian(stream_key, extent, width, bound, shards=(), kind=jnp.bfloat16):
    level = block_scale(stream_key, extent, shards, -0.22, 0.18) if shards else 1.0
    drawn = jax.random.normal(stream_key, extent, jnp.float32) * width * level
    return jnp.minimum(jnp.maximum(drawn, -bound), bound).astype(kind)


def setup_inputs(seed: int = 0) -> dict:
    key_list = jax.random.split(jax.random.key(seed), 17)
    tokens = gaussian(key_list[0], (TOKEN_TOTAL, MODEL_DIMENSION), 1.0, 6.0, ((0, 8),))
    cotangent = draw_cotangent(jax.random.fold_in(key_list[16], 71), 0)
    seq_start = draw_seq_start(jax.random.fold_in(key_list[16], 71), 0)
    routes_keys = jax.random.split(jax.random.fold_in(key_list[3], 1), TOKEN_TOTAL // TOKENS_PER_SHARD)
    routes_turns = jax.random.permutation(jax.random.fold_in(key_list[3], 3), TOKEN_TOTAL // TOKENS_PER_SHARD)
    routes = jax.vmap(lambda own, number: shared_out(jax.random.fold_in(key_list[3], 2), own, number, TOKENS_PER_SHARD, EXPERTS, TOPK, CAP, 2))(routes_keys, routes_turns).reshape((TOKEN_TOTAL, TOPK))
    norm1_gain = jnp.clip(1.0 + 0.15 * jax.random.normal(key_list[4], (MODEL_DIMENSION,), jnp.float32), 0.25, 1.75)
    norm2_gain = jnp.clip(1.0 + 0.15 * jax.random.normal(key_list[5], (MODEL_DIMENSION,), jnp.float32), 0.25, 1.75)
    q_gain = jnp.clip(1.0 + 0.15 * jax.random.normal(key_list[6], (HEAD_DIMENSION,), jnp.float32), 0.25, 1.75)
    k_gain = jnp.clip(1.0 + 0.15 * jax.random.normal(key_list[7], (HEAD_DIMENSION,), jnp.float32), 0.25, 1.75)
    query_matrix = gaussian(key_list[8], (MODEL_DIMENSION, QUERY_HEADS * HEAD_DIMENSION), MODEL_DIMENSION ** -0.5, 0.125, ((1, 4),))
    key_matrix = gaussian(key_list[9], (MODEL_DIMENSION, KEY_VALUE_HEADS * HEAD_DIMENSION), MODEL_DIMENSION ** -0.5, 0.125, ((1, 4),))
    value_matrix = gaussian(key_list[10], (MODEL_DIMENSION, KEY_VALUE_HEADS * HEAD_DIMENSION), MODEL_DIMENSION ** -0.5, 0.125, ((1, 4),))
    output_matrix = gaussian(key_list[11], (MODEL_DIMENSION, QUERY_HEADS * HEAD_DIMENSION), (QUERY_HEADS * HEAD_DIMENSION // 64) ** -0.5, 0.75, ((1, 4),))
    w_router = gaussian(key_list[12], (MODEL_DIMENSION, EXPERTS), MODEL_DIMENSION ** -0.5, 0.125)
    w_gate = gaussian(key_list[13], (EXPERTS, MODEL_DIMENSION, FFE), MODEL_DIMENSION ** -0.5, 0.125, ((0, 8), (2, 4)))
    w_up = gaussian(key_list[14], (EXPERTS, MODEL_DIMENSION, FFE), MODEL_DIMENSION ** -0.5, 0.125, ((0, 8), (2, 4)))
    w_down = gaussian(key_list[15], (EXPERTS, FFE, MODEL_DIMENSION), (FFE // 4) ** -0.5, 0.4375, ((0, 8), (1, 4)))
    return {"tokens": tokens, "cotangent": cotangent, "seq_start": seq_start, "routes": routes, "norm1_gain": norm1_gain, "norm2_gain": norm2_gain, "q_gain": q_gain, "k_gain": k_gain, "query_matrix": query_matrix, "key_matrix": key_matrix, "value_matrix": value_matrix, "output_matrix": output_matrix, "w_router": w_router, "w_gate": w_gate, "w_up": w_up, "w_down": w_down}


EPSILON = 1e-06
ROPE_BASE = 1000000.0
MASKED = -1e+30

def rotate_normed(pre_proj, gain_vec, positions):
    normed = pre_proj * lax.rsqrt(lax.optimization_barrier(jnp.mean(pre_proj * pre_proj, -1, keepdims=True)) + EPSILON) * gain_vec
    half_dim = HEAD_DIMENSION // 2
    freqs = ROPE_BASE ** (-(jnp.arange(half_dim).astype(jnp.float32) * 2.0 / HEAD_DIMENSION))
    angles = positions.reshape((-1,) + (1,) * (normed.ndim - 2) + (1,)) * freqs
    cosine = jnp.cos(angles)
    sine = jnp.sin(angles)
    first_half = normed[..., :half_dim]
    second_half = normed[..., half_dim:]
    return jnp.concatenate([first_half * cosine - second_half * sine, second_half * cosine + first_half * sine], -1)

def masked_scores(query_blk, key_rot, query_rows, query_start, key_start):
    scores = jnp.einsum('igrd,jgd->grij', query_blk.astype(jnp.float32), key_rot.astype(jnp.float32)) * HEAD_DIMENSION ** (-0.5)
    key_rows = jnp.arange(key_rot.shape[0])
    allowed = (key_rows[None, :] <= query_rows[:, None]) & (key_start[None, :] == query_start[:, None])
    return jnp.where(allowed[None, None], scores, MASKED)

def attend_forward(query_rot, key_rot, value_half_precision, query_rows, query_start, key_start):
    scores = masked_scores(query_rot, key_rot, query_rows, query_start, key_start)
    peak = lax.optimization_barrier(jnp.max(scores, -1, keepdims=True))
    weights = jnp.exp(scores - peak)
    totals = lax.optimization_barrier(jnp.sum(weights, -1, keepdims=True))
    log_total = (peak + jnp.log(totals))[..., 0]
    probs = (weights / totals).astype(jnp.bfloat16)
    attended = jnp.einsum('grij,jgd->igrd', probs.astype(jnp.float32), value_half_precision.astype(jnp.float32))
    return (attended.astype(jnp.bfloat16), log_total)

def attend_backward(query_rot, key_rot, value_half_precision, attended_bf, log_total, grad_att, query_rows, query_start, key_start):
    scores = masked_scores(query_rot, key_rot, query_rows, query_start, key_start)
    probs = jnp.exp(scores - log_total[..., None])
    probs_bf = probs.astype(jnp.bfloat16)
    grad_att_f = grad_att.astype(jnp.float32)
    grad_value = jnp.einsum('grij,igrd->jgd', probs_bf.astype(jnp.float32), grad_att_f)
    grad_probs = jnp.einsum('igrd,jgd->grij', grad_att_f, value_half_precision.astype(jnp.float32))
    delta = lax.optimization_barrier(jnp.sum(grad_att_f * attended_bf.astype(jnp.float32), -1))
    grad_scores = (probs * (grad_probs - jnp.transpose(delta, (1, 2, 0))[..., None])).astype(jnp.bfloat16)
    scale = HEAD_DIMENSION ** (-0.5)
    grad_query = jnp.einsum('grij,jgd->igrd', grad_scores.astype(jnp.float32), key_rot.astype(jnp.float32)) * scale
    grad_key = jnp.einsum('grij,igrd->jgd', grad_scores.astype(jnp.float32), query_rot.astype(jnp.float32)) * scale
    return (grad_query, grad_key, grad_value)

def reference(tokens, cotangent, seq_start, routes, norm1_gain, norm2_gain, q_gain, k_gain, query_matrix, key_matrix, value_matrix, output_matrix, w_router, w_gate, w_up, w_down):
    block_list = N_EXP
    group_repeats = QUERY_HEADS // KEY_VALUE_HEADS
    cap_total = N_EXP * CAP
    resid = tokens.astype(jnp.float32)
    scale_one = lax.rsqrt(lax.optimization_barrier(jnp.mean(resid * resid, -1, keepdims=True)) + EPSILON)
    first_normalized = (resid * scale_one * norm1_gain).astype(jnp.bfloat16)
    query_before_norm = jnp.dot(first_normalized, query_matrix, preferred_element_type=jnp.float32).reshape(block_list, TOKENS_PER_SHARD, KEY_VALUE_HEADS, group_repeats, HEAD_DIMENSION)
    key_before_norm = jnp.dot(first_normalized, key_matrix, preferred_element_type=jnp.float32).reshape(block_list, TOKENS_PER_SHARD, KEY_VALUE_HEADS, HEAD_DIMENSION)
    value_half_precision = jnp.dot(first_normalized, value_matrix, preferred_element_type=jnp.float32).astype(jnp.bfloat16).reshape(block_list, TOKENS_PER_SHARD, KEY_VALUE_HEADS, HEAD_DIMENSION)
    starts = seq_start.reshape(block_list, TOKENS_PER_SHARD)
    local_rows = jnp.arange(TOKENS_PER_SHARD)

    def forward_block(carry, inputs):
        q_blk, k_blk, v_blk, start_blk = inputs
        positions = (local_rows - start_blk).astype(jnp.float32)
        q_rot = rotate_normed(q_blk, q_gain, positions).astype(jnp.bfloat16)
        k_rot = rotate_normed(k_blk, k_gain, positions).astype(jnp.bfloat16)
        attended, log_total = attend_forward(q_rot, k_rot, v_blk, local_rows, start_blk, start_blk)
        return (carry, (attended, log_total))
    _, (attended_bf, log_totals) = lax.scan(forward_block, jnp.zeros((), jnp.float32), (query_before_norm, key_before_norm, value_half_precision, starts))
    attended_flat = attended_bf.reshape(TOKEN_TOTAL, QUERY_HEADS * HEAD_DIMENSION)
    after_attn = resid + jnp.dot(attended_flat, output_matrix.T, preferred_element_type=jnp.float32)
    scale_two = lax.rsqrt(lax.optimization_barrier(jnp.mean(after_attn * after_attn, -1, keepdims=True)) + EPSILON)
    normed_two = (after_attn * scale_two * norm2_gain).astype(jnp.bfloat16)
    logits = jnp.dot(normed_two, w_router, preferred_element_type=jnp.float32)
    chosen = jnp.take_along_axis(logits, routes, 1)
    gates = jax.nn.softmax(chosen, -1)
    flat_routes = routes.reshape(-1)
    one_hot = (flat_routes[:, None] == jnp.arange(EXPERTS)[None, :]).astype(jnp.int32)
    running = jnp.cumsum(one_hot.reshape(block_list, TOKENS_PER_SHARD * TOPK, EXPERTS), 1).reshape(-1, EXPERTS)
    slots = lax.optimization_barrier(jnp.sum(running * one_hot, 1)) - 1
    block_ids = jnp.arange(TOKEN_TOTAL * TOPK) // (TOKENS_PER_SHARD * TOPK)
    places = (flat_routes * cap_total + block_ids * CAP + slots).astype(jnp.int32)
    expert_in = jnp.zeros((EXPERTS * cap_total, MODEL_DIMENSION), jnp.bfloat16).at[places].set(jnp.repeat(normed_two, TOPK, 0)).reshape(EXPERTS, cap_total, MODEL_DIMENSION)
    grad_y = cotangent.astype(jnp.float32)
    expert_grad = (gates[..., None] * grad_y[:, None, :]).astype(jnp.bfloat16).reshape(TOKEN_TOTAL * TOPK, MODEL_DIMENSION)
    expert_grad_in = jnp.zeros((EXPERTS * cap_total, MODEL_DIMENSION), jnp.bfloat16).at[places].set(expert_grad).reshape(EXPERTS, cap_total, MODEL_DIMENSION)
    share = FFE // N_TP
    contract_last = (((1,), (1,)), ((), ()))
    contract_first = (((0,), (0,)), ((), ()))

    def expert_step(carry, inputs):
        rows_in, grads_in, gate_w, up_w, down_w = inputs
        gate_pre = jnp.dot(rows_in, gate_w, preferred_element_type=jnp.float32)
        up_pre = jnp.dot(rows_in, up_w, preferred_element_type=jnp.float32)
        sigmoid_g = jax.nn.sigmoid(gate_pre)
        silu_g = gate_pre * sigmoid_g
        hidden = (silu_g * up_pre).astype(jnp.bfloat16)
        grad_hidden = lax.dot_general(grads_in, down_w, contract_last, preferred_element_type=jnp.float32)
        grad_gate_pre = (grad_hidden * up_pre * sigmoid_g * (1.0 + gate_pre * (1.0 - sigmoid_g))).astype(jnp.bfloat16)
        grad_up_pre = (grad_hidden * silu_g).astype(jnp.bfloat16)
        outputs_sum = jnp.zeros((rows_in.shape[0], MODEL_DIMENSION), jnp.float32)
        back_sum = jnp.zeros((rows_in.shape[0], MODEL_DIMENSION), jnp.float32)
        for part_index in range(N_TP):
            low_col = part_index * share
            high_col = low_col + share
            piece_out = jnp.dot(hidden[:, low_col:high_col], down_w[low_col:high_col], preferred_element_type=jnp.float32)
            outputs_sum = outputs_sum + lax.optimization_barrier(piece_out.astype(jnp.bfloat16)).astype(jnp.float32)
            piece_back = lax.dot_general(grad_gate_pre[:, low_col:high_col], gate_w[:, low_col:high_col], contract_last, preferred_element_type=jnp.float32)
            piece_back = piece_back + lax.dot_general(grad_up_pre[:, low_col:high_col], up_w[:, low_col:high_col], contract_last, preferred_element_type=jnp.float32)
            back_sum = back_sum + lax.optimization_barrier(piece_back.astype(jnp.bfloat16)).astype(jnp.float32)
        grad_gate_w = lax.dot_general(rows_in, grad_gate_pre, contract_first, preferred_element_type=jnp.float32)
        grad_up_w = lax.dot_general(rows_in, grad_up_pre, contract_first, preferred_element_type=jnp.float32)
        grad_down_w = lax.dot_general(hidden, grads_in, contract_first, preferred_element_type=jnp.float32)
        return (carry, (outputs_sum, back_sum, grad_gate_w, grad_up_w, grad_down_w))
    _, (expert_out, expert_back, grad_gate, grad_up, grad_down) = lax.scan(expert_step, jnp.zeros((), jnp.float32), (expert_in, expert_grad_in, w_gate, w_up, w_down))
    picked = expert_out.reshape(EXPERTS * cap_total, MODEL_DIMENSION)[places].reshape(TOKEN_TOTAL, TOPK, MODEL_DIMENSION)
    mixture = lax.optimization_barrier(jnp.sum(gates[..., None] * picked, 1))
    layer_out = (after_attn + mixture).astype(jnp.bfloat16)
    grad_gates = lax.optimization_barrier(jnp.sum(grad_y[:, None, :] * picked, -1))
    grad_chosen = gates * (grad_gates - lax.optimization_barrier(jnp.sum(gates * grad_gates, -1, keepdims=True)))
    grad_logits = lax.optimization_barrier(jnp.sum((routes[:, :, None] == jnp.arange(EXPERTS)[None, None, :]).astype(jnp.float32) * grad_chosen[..., None], 1)).astype(jnp.bfloat16)
    grad_router = lax.dot_general(normed_two, grad_logits, contract_first, preferred_element_type=jnp.float32)
    returned = expert_back.reshape(EXPERTS * cap_total, MODEL_DIMENSION)[places].reshape(TOKEN_TOTAL, TOPK, MODEL_DIMENSION)
    grad_normed_two = lax.optimization_barrier(jnp.sum(returned, 1)) + lax.dot_general(grad_logits, w_router, contract_last, preferred_element_type=jnp.float32)
    gain2_scaled = grad_normed_two * norm2_gain
    grad_norm2 = lax.optimization_barrier(jnp.sum(grad_normed_two * after_attn * scale_two, 0))
    grad_resid = grad_y + scale_two * gain2_scaled - after_attn * scale_two ** 3 * lax.optimization_barrier(jnp.mean(gain2_scaled * after_attn, -1, keepdims=True))
    residual_gradient_half = grad_resid.astype(jnp.bfloat16)
    grad_out = lax.dot_general(residual_gradient_half, attended_flat, contract_first, preferred_element_type=jnp.float32)
    attended_gradient = jnp.dot(residual_gradient_half, output_matrix, preferred_element_type=jnp.float32).astype(jnp.bfloat16).reshape(block_list, TOKENS_PER_SHARD, KEY_VALUE_HEADS, group_repeats, HEAD_DIMENSION)

    def backward_block(carry, inputs):
        q_blk, k_blk, v_blk, start_blk, att_blk, lse_blk, gatt_blk = inputs
        positions = (local_rows - start_blk).astype(jnp.float32)
        q_rot, q_back = jax.vjp(lambda pre_vals, gain_vals: rotate_normed(pre_vals, gain_vals, positions), q_blk, q_gain)
        k_rot, k_back = jax.vjp(lambda pre_vals, gain_vals: rotate_normed(pre_vals, gain_vals, positions), k_blk, k_gain)
        grad_q_rot, grad_k_rot, grad_v = attend_backward(q_rot.astype(jnp.bfloat16), k_rot.astype(jnp.bfloat16), v_blk, att_blk, lse_blk, gatt_blk, local_rows, start_blk, start_blk)
        grad_q_pre, grad_qg = q_back(grad_q_rot)
        grad_k_pre, grad_kg = k_back(grad_k_rot)
        return ((carry[0] + grad_qg, carry[1] + grad_kg), (grad_q_pre, grad_k_pre, grad_v))
    gain_zero = (jnp.zeros((HEAD_DIMENSION,), jnp.float32), jnp.zeros((HEAD_DIMENSION,), jnp.float32))
    (grad_q_gain, grad_k_gain), (grad_q_all, key_gradient_total, value_gradient_total) = lax.scan(backward_block, gain_zero, (query_before_norm, key_before_norm, value_half_precision, starts, attended_bf, log_totals, attended_gradient))
    grad_query_bf = grad_q_all.reshape(TOKEN_TOTAL, QUERY_HEADS * HEAD_DIMENSION).astype(jnp.bfloat16)
    key_gradient_half = key_gradient_total.reshape(TOKEN_TOTAL, KEY_VALUE_HEADS * HEAD_DIMENSION).astype(jnp.bfloat16)
    value_gradient_half = value_gradient_total.reshape(TOKEN_TOTAL, KEY_VALUE_HEADS * HEAD_DIMENSION).astype(jnp.bfloat16)
    grad_query = lax.dot_general(first_normalized, grad_query_bf, contract_first, preferred_element_type=jnp.float32)
    grad_key = lax.dot_general(first_normalized, key_gradient_half, contract_first, preferred_element_type=jnp.float32)
    grad_value = lax.dot_general(first_normalized, value_gradient_half, contract_first, preferred_element_type=jnp.float32)
    grad_normed_one = lax.dot_general(grad_query_bf, query_matrix, contract_last, preferred_element_type=jnp.float32)
    grad_normed_one = grad_normed_one + lax.dot_general(key_gradient_half, key_matrix, contract_last, preferred_element_type=jnp.float32)
    grad_normed_one = grad_normed_one + lax.dot_general(value_gradient_half, value_matrix, contract_last, preferred_element_type=jnp.float32)
    gain1_scaled = grad_normed_one * norm1_gain
    grad_norm1 = lax.optimization_barrier(jnp.sum(grad_normed_one * resid * scale_one, 0))
    grad_tokens = (grad_resid + scale_one * gain1_scaled - resid * scale_one ** 3 * lax.optimization_barrier(jnp.mean(gain1_scaled * resid, -1, keepdims=True))).astype(jnp.bfloat16)
    return (layer_out, grad_tokens, grad_norm1, grad_norm2, grad_q_gain, grad_k_gain, grad_query, grad_key, grad_value, grad_out, grad_router, grad_gate, grad_up, grad_down)
```

```python
import jax
import jax.numpy as jnp
from jax import lax
from jax.sharding import PartitionSpec as P

HEAD_DIMENSION = 128
EPSILON = 1e-06
ROPE_BASE = 1000000.0
MASKED = -1e30
F32 = jnp.float32
BF = jnp.bfloat16
LAST = (((1,), (1,)), ((), ()))
FIRST = (((0,), (0,)), ((), ()))


def dot(a, b, dims=(((1,), (0,)), ((), ()))):
    return lax.dot_general(a, b, dims, preferred_element_type=F32)


def rotate_normed(pre_proj, gain_vec, cosine, sine):
    normed = (
        pre_proj * lax.rsqrt(jnp.mean(pre_proj * pre_proj, -1, keepdims=True) + EPSILON) * gain_vec
    )
    half_dim = HEAD_DIMENSION // 2
    first_half = normed[..., :half_dim]
    second_half = normed[..., half_dim:]
    return jnp.concatenate(
        [first_half * cosine - second_half * sine, second_half * cosine + first_half * sine], -1
    )


def body(
    tokens,
    cotangent,
    seq_start,
    routes,
    norm1_gain,
    norm2_gain,
    q_gain,
    k_gain,
    query_matrix,
    key_matrix,
    value_matrix,
    output_matrix,
    w_router,
    w_gate,
    w_up,
    w_down,
):
    rows, width = tokens.shape
    groups = key_matrix.shape[1] // HEAD_DIMENSION
    heads = query_matrix.shape[1] // HEAD_DIMENSION
    repeats = heads // groups
    all_experts = w_router.shape[1]
    local, _, share = w_gate.shape
    n_tp = lax.axis_size("tp")
    quarter = rows // n_tp
    t_id = lax.axis_index("tp")
    e_id = lax.axis_index("exp")
    both = ("exp", "tp")

    def my_rows(a):
        return lax.dynamic_slice_in_dim(a, t_id * quarter, quarter, 0)

    def gather_all(a):
        return lax.all_gather(a, both, axis=0, tiled=True)

    gy_all = gather_all(my_rows(cotangent))
    routes_all = lax.all_gather(routes, "exp", axis=0, tiled=True)

    w_gu = jnp.concatenate(
        [
            jnp.transpose(w_gate, (1, 0, 2)).reshape(width, local * share),
            jnp.transpose(w_up, (1, 0, 2)).reshape(width, local * share),
        ],
        1,
    )
    w_dn = w_down.reshape(local * share, width)

    resid = tokens.astype(F32)
    scale_one = lax.rsqrt(jnp.mean(resid * resid, -1, keepdims=True) + EPSILON)
    normed_one = (resid * scale_one * norm1_gain).astype(BF)
    half_dim = HEAD_DIMENSION // 2
    freqs = ROPE_BASE ** (-(jnp.arange(half_dim).astype(F32) * 2.0 / HEAD_DIMENSION))
    angles = (jnp.arange(rows) - seq_start).astype(F32)[:, None] * freqs
    cosine, sine = jnp.cos(angles), jnp.sin(angles)
    q_pre = dot(normed_one, query_matrix).reshape(rows, heads, HEAD_DIMENSION)
    q_pre = jnp.transpose(q_pre, (1, 0, 2)).reshape(groups, repeats, rows, HEAD_DIMENSION)
    k_pre = dot(normed_one, key_matrix).reshape(rows, groups, HEAD_DIMENSION)
    k_pre = jnp.transpose(k_pre, (1, 0, 2))
    value = dot(normed_one, value_matrix).astype(BF).reshape(rows, groups, HEAD_DIMENSION)
    value = jnp.transpose(value, (1, 0, 2))
    rot = lambda pre, gain: rotate_normed(pre, gain, cosine, sine)
    q_rot, q_back = jax.vjp(rot, q_pre, q_gain)
    k_rot, k_back = jax.vjp(rot, k_pre, k_gain)
    q_bf = q_rot.astype(BF)
    k_bf = k_rot.astype(BF)
    ids = jnp.arange(rows)
    allowed = (ids[None, :] <= ids[:, None]) & (seq_start[None, :] == seq_start[:, None])
    scores = jnp.einsum("grid,gjd->grij", q_bf, k_bf, preferred_element_type=F32)
    scores = jnp.where(allowed, scores * HEAD_DIMENSION ** (-0.5), MASKED)
    peak = jnp.max(scores, -1, keepdims=True)
    weights = jnp.exp(scores - peak)
    probs = weights / jnp.sum(weights, -1, keepdims=True)
    probs_bf = probs.astype(BF)
    attended = jnp.einsum("grij,gjd->grid", probs_bf, value, preferred_element_type=F32).astype(BF)
    att_flat = jnp.transpose(attended.reshape(heads, rows, HEAD_DIMENSION), (1, 0, 2)).reshape(
        rows, heads * HEAD_DIMENSION
    )
    attn_part = dot(att_flat, output_matrix, LAST)
    after = my_rows(tokens).astype(F32) + lax.psum_scatter(
        attn_part, "tp", scatter_dimension=0, tiled=True
    )
    scale_two = lax.rsqrt(jnp.mean(after * after, -1, keepdims=True) + EPSILON)
    normed_two = (after * scale_two * norm2_gain).astype(BF)
    x_all = gather_all(normed_two)

    logits = dot(x_all, w_router)
    named = jnp.any(routes_all[:, :, None] == jnp.arange(all_experts)[None, None, :], 1)
    logits = jnp.where(named, logits, MASKED)
    gexp = jnp.where(named, jnp.exp(logits - jnp.max(logits, -1, keepdims=True)), 0.0)
    gates = gexp / jnp.sum(gexp, -1, keepdims=True)
    mine = lax.dynamic_slice_in_dim(gates, e_id * local, local, 1)
    wide = jnp.repeat(mine, share, axis=1)
    pre = dot(x_all, w_gu)
    gate_pre, up_pre = pre[:, : local * share], pre[:, local * share :]
    g_hidden = dot(gy_all, w_dn, LAST)
    sig = jax.nn.sigmoid(gate_pre)
    silu = gate_pre * sig
    hidden = silu * up_pre
    gates_part = jnp.sum((hidden * g_hidden).reshape(-1, local, share), -1)
    gated_hidden = (wide * hidden).astype(BF)
    mix_part = dot(gated_hidden, w_dn).astype(BF)
    grad_hidden = wide * g_hidden
    grad_gate_pre = grad_hidden * up_pre * sig * (1.0 + gate_pre * (1.0 - sig))
    grad_up_pre = grad_hidden * silu
    grad_pre = jnp.concatenate([grad_gate_pre, grad_up_pre], 1).astype(BF)
    dx_part = dot(grad_pre, w_gu, LAST).astype(BF)

    gg = lax.all_to_all(gates_part, "exp", split_axis=0, concat_axis=1, tiled=True)
    grad_gates = lax.psum_scatter(gg, "tp", scatter_dimension=0, tiled=True)
    my_gates = lax.dynamic_slice_in_dim(gates, (e_id * n_tp + t_id) * quarter, quarter, 0)
    grad_logits = (
        my_gates * (grad_gates - jnp.sum(my_gates * grad_gates, -1, keepdims=True))
    ).astype(BF)
    glog_all = gather_all(grad_logits)

    dx = lax.psum_scatter(dx_part, both, scatter_dimension=0, tiled=True).astype(F32)
    mixture = lax.psum_scatter(mix_part, both, scatter_dimension=0, tiled=True).astype(F32)
    layer_out = lax.all_gather((after + mixture).astype(BF), "tp", axis=0, tiled=True)

    grad_n2 = dx + dot(grad_logits, w_router, LAST)
    gain2 = grad_n2 * norm2_gain
    norm2_part = jnp.sum(grad_n2 * after * scale_two, 0)
    grad_resid = (
        my_rows(cotangent).astype(F32)
        + scale_two * gain2
        - after * scale_two**3 * jnp.mean(gain2 * after, -1, keepdims=True)
    )
    grad_resid_bf = lax.all_gather(grad_resid.astype(BF), "tp", axis=0, tiled=True)

    out_part = dot(grad_resid_bf, att_flat, FIRST)
    grad_att = dot(grad_resid_bf, output_matrix).astype(BF).reshape(rows, heads, HEAD_DIMENSION)
    grad_att = jnp.transpose(grad_att, (1, 0, 2)).reshape(groups, repeats, rows, HEAD_DIMENSION)
    grad_value = jnp.einsum("grij,grid->gjd", probs_bf, grad_att, preferred_element_type=F32)
    grad_probs = jnp.einsum("grid,gjd->grij", grad_att, value, preferred_element_type=F32)
    delta = jnp.sum(grad_att.astype(F32) * attended.astype(F32), -1, keepdims=True)
    grad_scores = (probs * (grad_probs - delta) ).astype(BF)
    scale = HEAD_DIMENSION ** (-0.5)
    grad_q = jnp.einsum("grij,gjd->grid", grad_scores, k_bf, preferred_element_type=F32) * scale
    grad_k = jnp.einsum("grij,grid->gjd", grad_scores, q_bf, preferred_element_type=F32) * scale
    gq_pre, q_gain_part = q_back(grad_q)
    gk_pre, k_gain_part = k_back(grad_k)
    flat = lambda a: jnp.transpose(a.reshape(-1, rows, HEAD_DIMENSION), (1, 0, 2)).reshape(rows, -1)
    gqkv = jnp.concatenate(
        [flat(gq_pre).astype(BF), flat(gk_pre).astype(BF), flat(grad_value).astype(BF)], 1
    )
    nq, nk = query_matrix.shape[1], key_matrix.shape[1]
    input_part = (
        dot(gqkv[:, :nq], query_matrix, LAST)
        + dot(gqkv[:, nq : nq + nk], key_matrix, LAST)
        + dot(gqkv[:, nq + nk :], value_matrix, LAST)
    )
    qkv_part = dot(normed_one, gqkv, FIRST)
    grad_n1 = lax.psum_scatter(
        input_part.astype(BF), "tp", scatter_dimension=0, tiled=True
    ).astype(F32)
    my_resid = my_rows(tokens).astype(F32)
    my_scale = my_rows(scale_one)
    gain1 = grad_n1 * norm1_gain
    norm1_part = jnp.sum(grad_n1 * my_resid * my_scale, 0)
    grad_tokens = (
        grad_resid
        + my_scale * gain1
        - my_resid * my_scale**3 * jnp.mean(gain1 * my_resid, -1, keepdims=True)
    ).astype(BF)
    grad_tokens = lax.all_gather(grad_tokens, "tp", axis=0, tiled=True)

    grad_out = lax.psum_scatter(
        out_part.astype(BF), "exp", scatter_dimension=0, tiled=True
    ).astype(F32)
    qkv = lax.psum_scatter(qkv_part.astype(BF), "exp", scatter_dimension=0, tiled=True).astype(F32)
    cols = width // lax.axis_size("exp")
    x_cols = lax.dynamic_slice_in_dim(x_all, e_id * cols, cols, 1)
    grad_router = dot(x_cols, glog_all, FIRST)
    small = jnp.concatenate([norm1_part, norm2_part, q_gain_part, k_gain_part])
    small = lax.psum(small, both)

    w_grad = dot(x_all, grad_pre, FIRST)
    down_grad = dot(gated_hidden, gy_all, FIRST)
    unfold = lambda a: jnp.transpose(a.reshape(width, local, share), (1, 0, 2))
    return (
        layer_out,
        grad_tokens,
        small[:width],
        small[width : 2 * width],
        small[2 * width : 2 * width + HEAD_DIMENSION],
        small[2 * width + HEAD_DIMENSION :],
        qkv[:, :nq],
        qkv[:, nq : nq + nk],
        qkv[:, nq + nk :],
        grad_out,
        grad_router,
        unfold(w_grad[:, : local * share]),
        unfold(w_grad[:, local * share :]),
        down_grad.reshape(local, share, width),
    )


def solution(mesh):
    e, t = "exp", "tp"
    return jax.shard_map(
        body,
        mesh=mesh,
        in_specs=(
            P(e, None), P(e, None), P(e), P(e, None), P(), P(), P(), P(),
            P(None, t), P(None, t), P(None, t), P(None, t), P(),
            P(e, None, t), P(e, None, t), P(e, t, None),
        ),
        out_specs=(
            P(e, None), P(e, None), P(), P(), P(), P(),
            P(e, t), P(e, t), P(e, t), P(e, t), P(e, None),
            P(e, None, t), P(e, None, t), P(e, t, None),
        ),
        check_vma=False,
    )
```

```python
import functools

import jax
import jax.numpy as jnp
from jax import lax
from jax.experimental import pallas as pl
from jax.experimental.pallas import tpu as pltpu
from jax.sharding import PartitionSpec as P

MESH = pl.DeviceIdType.MESH

HEAD_DIMENSION = 128
EPSILON = 1e-06
ROPE_BASE = 1000000.0
MASKED = -1e30
F32 = jnp.float32
BF = jnp.bfloat16
LAST = (((1,), (1,)), ((), ()))
FIRST = (((0,), (0,)), ((), ()))


def dot(a, b, dims=(((1,), (0,)), ((), ()))):
    return lax.dot_general(a, b, dims, preferred_element_type=F32)


def place():
    e, t = lax.axis_index("exp"), lax.axis_index("tp")
    return e // 2, e % 2, t // 2, t % 2

def dev(z, y, x, c):
    return (z * 2 + y, x * 2 + c)

def geometry():
    z, y, x, c = place()
    first = c == 0
    a, b = jnp.where(first, x, y), jnp.where(first, y, x)
    nbr_a = dev(z, jnp.where(first, y, 1 - y), jnp.where(first, 1 - x, x), c)
    nbr_b = dev(z, jnp.where(first, 1 - y, y), jnp.where(first, x, 1 - x), c)
    low = z < 2
    m = jnp.where(low, z, 3 - z)
    step = jnp.where(low, 1, -1)
    mir = lambda k: jnp.where(low, k, 3 - k)
    ahead = dev(z + step, y, x, c)
    back = dev(jnp.where(m == 0, z, z - step), y, x, c)
    return z, y, x, c, a, b, nbr_a, nbr_b, m, mir, ahead, back, dev(z, y, x, 1 - c)

def greet(ids, extra, extra_ok):
    barrier = pltpu.get_barrier_semaphore()
    for d in ids:
        pl.semaphore_signal(barrier, inc=1, device_id=d, device_id_type=MESH)
    @pl.when(extra_ok)
    def _():
        pl.semaphore_signal(barrier, inc=1, device_id=extra, device_id_type=MESH)
    pl.semaphore_wait(barrier, len(ids) + jnp.where(extra_ok, 1, 0))

def rcopy(src, dst, ss, rs, d):
    return pltpu.make_async_remote_copy(src_ref=src, dst_ref=dst, send_sem=ss, recv_sem=rs, device_id=d, device_id_type=MESH)

def rows_loop(n, step, fn):
    def it(i, _):
        fn(pl.ds(pl.multiple_of(i * step, step), step))
        return 0
    lax.fori_loop(0, n // step, it, 0)

def rs_kernel(part, out, own, prt, ra, r, rb, s_own, s_cs, s_cr, s_as, s_ar, s_zs, s_zr, s_bs, s_br):
    z, y, x, c, a, b, nbr_a, nbr_b, m, mir, ahead, back, mate = geometry()
    q = out.shape[0]
    block = 4 * q
    greet([mate, nbr_a, nbr_b, ahead], back, m == 1)
    order = [mir(3), mir(2), mir(jnp.where(m == 0, 1, 0)), z]

    def src(k, i, j, core):
        yy = jnp.where(core == 0, j, i)
        xx = jnp.where(core == 0, i, j)
        return part.at[pl.ds(pl.multiple_of((k * 2 + yy) * block + (xx * 2 + core) * q, q), q)]

    for n, k in enumerate(order):
        for i in range(2):
            for j in range(2):
                rcopy(src(k, i, j, 1 - c), prt.at[k, i, j], s_cs.at[n, i, j], s_cr.at[n, i, j], mate).start()
        for i in range(2):
            for j in range(2):
                pltpu.make_async_copy(src(k, i, j, c), own.at[k, i, j], s_own.at[n, i, j]).start()
    for n, k in enumerate(order):
        for i in range(2):
            for j in range(2):
                pltpu.make_async_copy(src(k, i, j, c), own.at[k, i, j], s_own.at[n, i, j]).wait()
                rcopy(src(k, i, j, 1 - c), prt.at[k, i, j], s_cs.at[n, i, j], s_cr.at[n, i, j], mate).wait()
        for j in range(2):
            def add(rows, j=j, k=k):
                own[k, 1 - a, j, rows, :] = (own[k, 1 - a, j, rows, :].astype(F32) + prt[k, 1 - a, j, rows, :].astype(F32)).astype(BF)
            rows_loop(q, 16, add)
        rcopy(own.at[k, 1 - a], ra.at[k], s_as.at[n], s_ar.at[n], nbr_a).start()
    for n, k in enumerate(order[:3]):
        rcopy(own.at[k, 1 - a], ra.at[k], s_as.at[n], s_ar.at[n], nbr_a).wait()
        slot_in = n
        def wait_r(k=k, n=n):
            rcopy(own.at[k, a], r.at[n], s_zs.at[n], s_zr.at[n], ahead).wait_recv()
        @pl.when(m == 1)
        def _(k=k, n=n):
            wait_r(k, n)
            for j in range(2):
                def add(rows, j=j):
                    own[k, a, j, rows, :] = (own[k, a, j, rows, :].astype(F32) + prt[k, a, j, rows, :].astype(F32)
                        + ra[k, j, rows, :].astype(F32) + r[n, j, rows, :].astype(F32)).astype(BF)
                rows_loop(q, 16, add)
        @pl.when(m == 0)
        def _(k=k, n=n):
            for j in range(2):
                def add(rows, j=j):
                    own[k, a, j, rows, :] = (own[k, a, j, rows, :].astype(F32) + prt[k, a, j, rows, :].astype(F32)
                        + ra[k, j, rows, :].astype(F32)).astype(BF)
                rows_loop(q, 16, add)
        if n < 2:
            slot = jnp.where(m == 0, n, n + 2)
            rcopy(own.at[k, a], r.at[slot], s_zs.at[n], s_zr.at[slot], ahead).start()
        else:
            @pl.when(m == 0)
            def _(k=k, n=n):
                rcopy(own.at[k, a], r.at[4], s_zs.at[n], s_zr.at[4], ahead).start()
            @pl.when(m == 1)
            def _(k=k, n=n):
                rcopy(own.at[k, a], r.at[3], s_zs.at[n], s_zr.at[3], back).start()
    k, n = z, 3
    rcopy(own.at[k, 1 - a], ra.at[k], s_as.at[n], s_ar.at[n], nbr_a).wait()
    rcopy(own.at[k, a], r.at[3], s_zs.at[0], s_zr.at[3], ahead).wait_recv()

    def total(j, rows):
        return (own[k, a, j, rows, :].astype(F32) + prt[k, a, j, rows, :].astype(F32)
            + ra[k, j, rows, :].astype(F32) + r[3, j, rows, :].astype(F32))
    @pl.when(m == 1)
    def _():
        rcopy(own.at[k, a], r.at[4], s_zs.at[0], s_zr.at[4], ahead).wait_recv()
        def add(rows):
            own[k, a, 1 - b, rows, :] = (total(1 - b, rows) + r[4, 1 - b, rows, :].astype(F32)).astype(BF)
        rows_loop(q, 16, add)
    @pl.when(m == 0)
    def _():
        def add(rows):
            own[k, a, 1 - b, rows, :] = total(1 - b, rows).astype(BF)
        rows_loop(q, 16, add)
    last = rcopy(own.at[k, a, 1 - b], rb, s_bs, s_br, nbr_b)
    last.start()
    @pl.when(m == 1)
    def _():
        def add(rows):
            out[rows, :] = total(b, rows) + r[4, b, rows, :].astype(F32)
        rows_loop(q, 16, add)
    @pl.when(m == 0)
    def _():
        def add(rows):
            out[rows, :] = total(b, rows)
        rows_loop(q, 16, add)
    last.wait()
    def add(rows):
        out[rows, :] = out[rows, :] + rb[rows, :].astype(F32)
    rows_loop(q, 16, add)
    for n, k in enumerate(order[:3]):
        rcopy(own.at[k, a], r.at[0], s_zs.at[n], s_zr.at[0], ahead).wait_send()

def reduce_scatter(part, cid):
    rows, width = part.shape
    q = rows // 32
    dma = lambda *s: pltpu.SemaphoreType.DMA(s)
    return pl.pallas_call(
        rs_kernel,
        out_shape=jax.ShapeDtypeStruct((q, width), F32),
        in_specs=[pl.BlockSpec(memory_space=pl.ANY)],
        out_specs=pl.BlockSpec(memory_space=pltpu.VMEM),
        scratch_shapes=[
            pltpu.VMEM((4, 2, 2, q, width), BF), pltpu.VMEM((4, 2, 2, q, width), BF),
            pltpu.VMEM((4, 2, q, width), BF), pltpu.VMEM((5, 2, q, width), BF), pltpu.VMEM((q, width), BF),
            dma(4, 2, 2), dma(4, 2, 2), dma(4, 2, 2), dma(4), dma(4), dma(3), dma(5),
            pltpu.SemaphoreType.DMA, pltpu.SemaphoreType.DMA,
        ],
        compiler_params=pltpu.CompilerParams(collective_id=cid, has_side_effects=True),
    )(part)


def rotate_normed(pre_proj, gain_vec, cosine, sine):
    normed = (
        pre_proj * lax.rsqrt(jnp.mean(pre_proj * pre_proj, -1, keepdims=True) + EPSILON) * gain_vec
    )
    half_dim = HEAD_DIMENSION // 2
    first_half = normed[..., :half_dim]
    second_half = normed[..., half_dim:]
    return jnp.concatenate(
        [first_half * cosine - second_half * sine, second_half * cosine + first_half * sine], -1
    )


def body(
    near,
    tokens,
    cotangent,
    seq_start,
    routes,
    norm1_gain,
    norm2_gain,
    q_gain,
    k_gain,
    query_matrix,
    key_matrix,
    value_matrix,
    output_matrix,
    w_router,
    w_gate,
    w_up,
    w_down,
):
    rows, width = tokens.shape
    groups = key_matrix.shape[1] // HEAD_DIMENSION
    heads = query_matrix.shape[1] // HEAD_DIMENSION
    repeats = heads // groups
    all_experts = w_router.shape[1]
    local, _, share = w_gate.shape
    n_tp = lax.axis_size("tp")
    quarter = rows // n_tp
    t_id = lax.axis_index("tp")
    e_id = lax.axis_index("exp")
    both = ("exp", "tp")

    def my_rows(a):
        return lax.dynamic_slice_in_dim(a, t_id * quarter, quarter, 0)

    def gather_all(a):
        return lax.all_gather(a, both, axis=0, tiled=True)

    gy_all = gather_all(my_rows(cotangent))
    routes_all = lax.all_gather(routes, "exp", axis=0, tiled=True)

    w_gu = jnp.concatenate(
        [
            jnp.transpose(w_gate, (1, 0, 2)).reshape(width, local * share),
            jnp.transpose(w_up, (1, 0, 2)).reshape(width, local * share),
        ],
        1,
    )
    w_dn = w_down.reshape(local * share, width)

    resid = tokens.astype(F32)
    scale_one = lax.rsqrt(jnp.mean(resid * resid, -1, keepdims=True) + EPSILON)
    normed_one = (resid * scale_one * norm1_gain).astype(BF)
    half_dim = HEAD_DIMENSION // 2
    freqs = ROPE_BASE ** (-(jnp.arange(half_dim).astype(F32) * 2.0 / HEAD_DIMENSION))
    angles = (jnp.arange(rows) - seq_start).astype(F32)[:, None] * freqs
    cosine, sine = jnp.cos(angles), jnp.sin(angles)
    q_pre = dot(normed_one, query_matrix).reshape(rows, heads, HEAD_DIMENSION)
    q_pre = jnp.transpose(q_pre, (1, 0, 2)).reshape(groups, repeats, rows, HEAD_DIMENSION)
    k_pre = dot(normed_one, key_matrix).reshape(rows, groups, HEAD_DIMENSION)
    k_pre = jnp.transpose(k_pre, (1, 0, 2))
    value = dot(normed_one, value_matrix).astype(BF).reshape(rows, groups, HEAD_DIMENSION)
    value = jnp.transpose(value, (1, 0, 2))
    rot = lambda pre, gain: rotate_normed(pre, gain, cosine, sine)
    q_rot, q_back = jax.vjp(rot, q_pre, q_gain)
    k_rot, k_back = jax.vjp(rot, k_pre, k_gain)
    q_bf = q_rot.astype(BF)
    k_bf = k_rot.astype(BF)
    ids = jnp.arange(rows)
    allowed = (ids[None, :] <= ids[:, None]) & (seq_start[None, :] == seq_start[:, None])
    scores = jnp.einsum("grid,gjd->grij", q_bf, k_bf, preferred_element_type=F32)
    scores = jnp.where(allowed, scores * HEAD_DIMENSION ** (-0.5), MASKED)
    peak = jnp.max(scores, -1, keepdims=True)
    weights = jnp.exp(scores - peak)
    probs = weights / jnp.sum(weights, -1, keepdims=True)
    probs_bf = probs.astype(BF)
    attended = jnp.einsum("grij,gjd->grid", probs_bf, value, preferred_element_type=F32).astype(BF)
    att_flat = jnp.transpose(attended.reshape(heads, rows, HEAD_DIMENSION), (1, 0, 2)).reshape(
        rows, heads * HEAD_DIMENSION
    )
    attn_part = dot(att_flat, output_matrix, LAST)
    after = my_rows(tokens).astype(F32) + lax.psum_scatter(
        attn_part, "tp", scatter_dimension=0, tiled=True
    )
    scale_two = lax.rsqrt(jnp.mean(after * after, -1, keepdims=True) + EPSILON)
    normed_two = (after * scale_two * norm2_gain).astype(BF)
    x_all = gather_all(normed_two)

    logits = dot(x_all, w_router)
    named = jnp.any(routes_all[:, :, None] == jnp.arange(all_experts)[None, None, :], 1)
    logits = jnp.where(named, logits, MASKED)
    gexp = jnp.where(named, jnp.exp(logits - jnp.max(logits, -1, keepdims=True)), 0.0)
    gates = gexp / jnp.sum(gexp, -1, keepdims=True)
    mine = lax.dynamic_slice_in_dim(gates, e_id * local, local, 1)
    wide = jnp.repeat(mine, share, axis=1)
    pre = dot(x_all, w_gu)
    gate_pre, up_pre = pre[:, : local * share], pre[:, local * share :]
    g_hidden = dot(gy_all, w_dn, LAST)
    sig = jax.nn.sigmoid(gate_pre)
    silu = gate_pre * sig
    hidden = silu * up_pre
    gates_part = jnp.sum((hidden * g_hidden).reshape(-1, local, share), -1)
    gated_hidden = (wide * hidden).astype(BF)
    mix_part = dot(gated_hidden, w_dn).astype(BF)
    grad_hidden = wide * g_hidden
    grad_gate_pre = grad_hidden * up_pre * sig * (1.0 + gate_pre * (1.0 - sig))
    grad_up_pre = grad_hidden * silu
    grad_pre = jnp.concatenate([grad_gate_pre, grad_up_pre], 1).astype(BF)
    dx_part = dot(grad_pre, w_gu, LAST).astype(BF)

    gg = lax.all_to_all(gates_part, "exp", split_axis=0, concat_axis=1, tiled=True)
    grad_gates = lax.psum_scatter(gg, "tp", scatter_dimension=0, tiled=True)
    my_gates = lax.dynamic_slice_in_dim(gates, (e_id * n_tp + t_id) * quarter, quarter, 0)
    grad_logits = (
        my_gates * (grad_gates - jnp.sum(my_gates * grad_gates, -1, keepdims=True))
    ).astype(BF)
    glog_all = gather_all(grad_logits)

    if near:
        dx = reduce_scatter(dx_part, 1)
        mixture = reduce_scatter(mix_part, 1)
    else:
        dx = lax.psum_scatter(dx_part, both, scatter_dimension=0, tiled=True).astype(F32)
        mixture = lax.psum_scatter(mix_part, both, scatter_dimension=0, tiled=True).astype(F32)
    layer_out = lax.all_gather((after + mixture).astype(BF), "tp", axis=0, tiled=True)

    grad_n2 = dx + dot(grad_logits, w_router, LAST)
    gain2 = grad_n2 * norm2_gain
    norm2_part = jnp.sum(grad_n2 * after * scale_two, 0)
    grad_resid = (
        my_rows(cotangent).astype(F32)
        + scale_two * gain2
        - after * scale_two**3 * jnp.mean(gain2 * after, -1, keepdims=True)
    )
    grad_resid_bf = lax.all_gather(grad_resid.astype(BF), "tp", axis=0, tiled=True)

    out_part = dot(grad_resid_bf, att_flat, FIRST)
    grad_att = dot(grad_resid_bf, output_matrix).astype(BF).reshape(rows, heads, HEAD_DIMENSION)
    grad_att = jnp.transpose(grad_att, (1, 0, 2)).reshape(groups, repeats, rows, HEAD_DIMENSION)
    grad_value = jnp.einsum("grij,grid->gjd", probs_bf, grad_att, preferred_element_type=F32)
    grad_probs = jnp.einsum("grid,gjd->grij", grad_att, value, preferred_element_type=F32)
    delta = jnp.sum(grad_att.astype(F32) * attended.astype(F32), -1, keepdims=True)
    grad_scores = (probs * (grad_probs - delta) ).astype(BF)
    scale = HEAD_DIMENSION ** (-0.5)
    grad_q = jnp.einsum("grij,gjd->grid", grad_scores, k_bf, preferred_element_type=F32) * scale
    grad_k = jnp.einsum("grij,grid->gjd", grad_scores, q_bf, preferred_element_type=F32) * scale
    gq_pre, q_gain_part = q_back(grad_q)
    gk_pre, k_gain_part = k_back(grad_k)
    flat = lambda a: jnp.transpose(a.reshape(-1, rows, HEAD_DIMENSION), (1, 0, 2)).reshape(rows, -1)
    gqkv = jnp.concatenate(
        [flat(gq_pre).astype(BF), flat(gk_pre).astype(BF), flat(grad_value).astype(BF)], 1
    )
    nq, nk = query_matrix.shape[1], key_matrix.shape[1]
    input_part = (
        dot(gqkv[:, :nq], query_matrix, LAST)
        + dot(gqkv[:, nq : nq + nk], key_matrix, LAST)
        + dot(gqkv[:, nq + nk :], value_matrix, LAST)
    )
    qkv_part = dot(normed_one, gqkv, FIRST)
    grad_n1 = lax.psum_scatter(
        input_part.astype(BF), "tp", scatter_dimension=0, tiled=True
    ).astype(F32)
    my_resid = my_rows(tokens).astype(F32)
    my_scale = my_rows(scale_one)
    gain1 = grad_n1 * norm1_gain
    norm1_part = jnp.sum(grad_n1 * my_resid * my_scale, 0)
    grad_tokens = (
        grad_resid
        + my_scale * gain1
        - my_resid * my_scale**3 * jnp.mean(gain1 * my_resid, -1, keepdims=True)
    ).astype(BF)
    grad_tokens = lax.all_gather(grad_tokens, "tp", axis=0, tiled=True)

    grad_out = lax.psum_scatter(
        out_part.astype(BF), "exp", scatter_dimension=0, tiled=True
    ).astype(F32)
    qkv = lax.psum_scatter(qkv_part.astype(BF), "exp", scatter_dimension=0, tiled=True).astype(F32)
    cols = width // lax.axis_size("exp")
    x_cols = lax.dynamic_slice_in_dim(x_all, e_id * cols, cols, 1)
    grad_router = dot(x_cols, glog_all, FIRST)
    small = jnp.concatenate([norm1_part, norm2_part, q_gain_part, k_gain_part])
    small = lax.psum(small, both)

    w_grad = dot(x_all, grad_pre, FIRST)
    down_grad = dot(gated_hidden, gy_all, FIRST)
    unfold = lambda a: jnp.transpose(a.reshape(width, local, share), (1, 0, 2))
    return (
        layer_out,
        grad_tokens,
        small[:width],
        small[width : 2 * width],
        small[2 * width : 2 * width + HEAD_DIMENSION],
        small[2 * width + HEAD_DIMENSION :],
        qkv[:, :nq],
        qkv[:, nq : nq + nk],
        qkv[:, nq + nk :],
        grad_out,
        grad_router,
        unfold(w_grad[:, : local * share]),
        unfold(w_grad[:, local * share :]),
        down_grad.reshape(local, share, width),
    )


def is_near(mesh):
    devices = mesh.devices
    if devices.shape != (8, 4):
        return False
    low = devices[0, 0].coords
    return all(
        tuple(p - o for p, o in zip(devices[e, t].coords, low)) + (devices[e, t].core_on_chip,)
        == (t // 2, e % 2, e // 2, t % 2)
        for e in range(8)
        for t in range(4)
    )


def solution(mesh):
    e, t = "exp", "tp"
    return jax.shard_map(
        functools.partial(body, is_near(mesh)),
        mesh=mesh,
        in_specs=(
            P(e, None), P(e, None), P(e), P(e, None), P(), P(), P(), P(),
            P(None, t), P(None, t), P(None, t), P(None, t), P(),
            P(e, None, t), P(e, None, t), P(e, t, None),
        ),
        out_specs=(
            P(e, None), P(e, None), P(), P(), P(), P(),
            P(e, t), P(e, t), P(e, t), P(e, t), P(e, None),
            P(e, None, t), P(e, None, t), P(e, t, None),
        ),
        check_vma=False,
    )
```
